64 devices in a mesh: dp: 8 (over x, y, core), tp: 8 (over z).
Axes of the slice: x: 2, y: 2, z: 8, core: 2. Of those that a mesh axis runs over, the one named last changes fastest.
The devices are a block of a 4x4x8 slice.
Arguments:
- x: bfloat16 [16384, 4096], P('dp'), parts along dimension 0
- w_gate: bfloat16 [4096, 14336], P(None, 'tp')
- w_up: bfloat16 [4096, 14336], P(None, 'tp')
- w_down: bfloat16 [14336, 4096], P('tp')
Outputs:
- output: bfloat16 [16384, 4096], P('dp'), parts along dimension 0
There are 8 independent parts. The reference program is written for one: setup_inputs(seed, part) draws one part's arguments, and reference() takes and returns one part's arrays. A program takes and returns all parts, laid end to end along the dimension named above; an argument that names none is the same for every part.
All inputs are finite; a program needn't handle non-finite values.
Results may differ from the reference program's by a relative error of at most 0.016.
Values are sent between devices in bfloat16 or wider.
A program may use at most 768 MiB of HBM per device.

```python
import jax
import jax.numpy as jnp

ROWS = 2048
D = 4096
FF = 14336


def setup_inputs(seed: int = 0, part: int = 0) -> dict:
    kx, kg, ku, kd = jax.random.split(jax.random.key(seed), 4)
    drawn = {
        "x": jax.random.normal(jax.random.fold_in(kx, part), (ROWS, D), jnp.float32),
        "w_gate": jax.random.normal(kg, (D, FF), jnp.float32) * D**-0.5,
        "w_up": jax.random.normal(ku, (D, FF), jnp.float32) * D**-0.5,
        "w_down": jax.random.normal(kd, (FF, D), jnp.float32) * FF**-0.5,
    }
    return {k: v.astype(jnp.bfloat16) for k, v in drawn.items()}


def reference(x, w_gate, w_up, w_down):
    gate = jnp.dot(x, w_gate, preferred_element_type=jnp.float32)
    up = jnp.dot(x, w_up, preferred_element_type=jnp.float32)
    hidden = (jax.nn.silu(gate) * up).astype(jnp.bfloat16)
    return jnp.dot(hidden, w_down, preferred_element_type=jnp.float32).astype(jnp.bfloat16)
```

```python
import functools

import jax
import jax.numpy as jnp
from jax import lax
from jax.experimental import pallas as pl
from jax.experimental.pallas import tpu as pltpu
from jax.sharding import PartitionSpec as P

MESH = pl.DeviceIdType.MESH
AXIS = "tp"


def kernel(
    n, x_hbm, wg_hbm, wu_hbm, wd_hbm, y, xv, wg, wu, wd, hidden, x_sem, up_sem, down_sem, send_sem, recv_sem
):
    me = lax.axis_index(AXIS)
    right, left = lax.rem(me + 1, n), lax.rem(me + n - 1, n)
    half = xv.shape[0] // 2
    up_tiles, _, up_tile = wg.shape
    down_tiles, _, down_tile = wd.shape

    def shard(direction, step):
        if direction == 0:
            return lax.rem(me + 2 * n - 1 - step, n)
        return lax.rem(me + 1 + step, n)

    def rows(direction, j):
        return pl.ds(pl.multiple_of(j * 2 * half + direction * half, half), half)

    def x_copy(direction, step):
        return pltpu.make_async_copy(
            x_hbm.at[rows(direction, shard(direction, step)), :],
            xv.at[pl.ds(direction * half, half), :],
            x_sem.at[direction],
        )

    def up_copies(t):
        columns = pl.ds(pl.multiple_of(t * up_tile, up_tile), up_tile)
        return [
            pltpu.make_async_copy(hbm.at[:, columns], vmem.at[t], up_sem.at[k, t])
            for k, (hbm, vmem) in enumerate(((wg_hbm, wg), (wu_hbm, wu)))
        ]

    def down_copy(t):
        columns = pl.ds(pl.multiple_of(t * down_tile, down_tile), down_tile)
        return pltpu.make_async_copy(wd_hbm.at[:, columns], wd.at[t], down_sem.at[t])

    def hop(direction, j, t):
        block = y.at[rows(direction, j), pl.ds(pl.multiple_of(t * down_tile, down_tile), down_tile)]
        return pltpu.make_async_remote_copy(
            src_ref=block,
            dst_ref=block,
            send_sem=send_sem.at[direction, j, t],
            recv_sem=recv_sem.at[direction, j, t],
            device_id={AXIS: right if direction == 0 else left},
            device_id_type=MESH,
        )

    def project_up(first):
        def tile(t, _):
            if first:
                for copy in up_copies(t):
                    copy.wait()
            gate = jnp.dot(xv[...], wg[t], preferred_element_type=jnp.float32)
            up = jnp.dot(xv[...], wu[t], preferred_element_type=jnp.float32)
            columns = pl.ds(pl.multiple_of(t * up_tile, up_tile), up_tile)
            hidden[:, columns] = (jax.nn.silu(gate) * up).astype(hidden.dtype)
            return 0

        lax.fori_loop(0, up_tiles, tile, 0)

    def project_down(first, step):
        js = [shard(d, step) for d in (0, 1)]
        before = [shard(d, step - 1) for d in (0, 1)]

        def tile(t, _):
            if first:
                down_copy(t).wait()
            term = jnp.dot(hidden[...], wd[t], preferred_element_type=jnp.float32)
            columns = pl.ds(pl.multiple_of(t * down_tile, down_tile), down_tile)
            for d in (0, 1):
                total = term[d * half : (d + 1) * half, :]
                if not first:
                    hop(d, js[d], t).wait_recv()
                    hop(d, before[d], t).wait_send()
                    total = total + y[rows(d, js[d]), columns].astype(jnp.float32)
                y[rows(d, js[d]), columns] = total.astype(y.dtype)

            @pl.when(t > 0)
            def _():
                for d in (0, 1):
                    hop(d, js[d], t - 1).start()

            return 0

        lax.fori_loop(0, down_tiles, tile, 0)
        for d in (0, 1):
            hop(d, js[d], down_tiles - 1).start()

    barrier = pltpu.get_barrier_semaphore()
    for neighbour in (left, right):
        pl.semaphore_signal(barrier, inc=1, device_id={AXIS: neighbour}, device_id_type=MESH)

    for d in (0, 1):
        x_copy(d, 0).start()

    def start_up(t, _):
        for copy in up_copies(t):
            copy.start()
        return 0

    lax.fori_loop(0, up_tiles, start_up, 0)

    def start_down(t, _):
        down_copy(t).start()
        return 0

    lax.fori_loop(0, down_tiles, start_down, 0)

    for d in (0, 1):
        x_copy(d, 0).wait()
    project_up(True)
    for d in (0, 1):
        x_copy(d, 1).start()
    pl.semaphore_wait(barrier, 2)
    project_down(True, 0)

    def reduce_step(step, _):
        for d in (0, 1):
            x_copy(d, step).wait()
        project_up(False)

        @pl.when(step < n - 1)
        def _():
            for d in (0, 1):
                x_copy(d, step + 1).start()

        project_down(False, step)
        return 0

    lax.fori_loop(1, n, reduce_step, 0)

    def gather_step(step, _):
        js = [lax.rem(me + n - step, n), lax.rem(me + step, n)]
        before = [lax.rem(me + n - step + 1, n), lax.rem(me + step - 1, n)]

        def tile(t, _):
            for d in (0, 1):
                hop(d, js[d], t).wait_recv()

                @pl.when(step < n - 1)
                def _():
                    hop(d, js[d], t).start()

                hop(d, before[d], t).wait_send()
            return 0

        return lax.fori_loop(0, down_tiles, tile, 0)

    lax.fori_loop(1, n, gather_step, 0)


def solution(mesh):
    n = mesh.shape[AXIS]

    def step(x, w_gate, w_up, w_down):
        tokens, d_model = x.shape
        hidden = w_gate.shape[1]
        block = tokens // n
        up_tile, down_tile = 256, 512
        up_tiles, down_tiles = hidden // up_tile, d_model // down_tile
        y = pl.pallas_call(
            functools.partial(kernel, n),
            out_shape=pltpu.VMEM((tokens, d_model), jnp.bfloat16),
            in_specs=[pl.BlockSpec(memory_space=pl.ANY)] * 4,
            out_specs=pl.BlockSpec(memory_space=pltpu.VMEM),
            scratch_shapes=[
                pltpu.VMEM((block, d_model), jnp.bfloat16),
                pltpu.VMEM((up_tiles, d_model, up_tile), jnp.bfloat16),
                pltpu.VMEM((up_tiles, d_model, up_tile), jnp.bfloat16),
                pltpu.VMEM((down_tiles, hidden, down_tile), jnp.bfloat16),
                pltpu.VMEM((block, hidden), jnp.bfloat16),
                pltpu.SemaphoreType.DMA((2,)),
                pltpu.SemaphoreType.DMA((2, up_tiles)),
                pltpu.SemaphoreType.DMA((down_tiles,)),
                pltpu.SemaphoreType.DMA((2, n, down_tiles)),
                pltpu.SemaphoreType.DMA((2, n, down_tiles)),
            ],
            compiler_params=pltpu.CompilerParams(
                collective_id=0, has_side_effects=True, vmem_limit_bytes=47 << 20
            ),
            name="mlp_ring",
        )(x, w_gate, w_up, w_down)
        return y

    return jax.shard_map(
        step,
        mesh=mesh,
        in_specs=(P("dp", None), P(None, AXIS), P(None, AXIS), P(AXIS, None)),
        out_specs=P("dp", None),
        check_vma=False,
    )
```

```python
import functools

import jax
import jax.numpy as jnp
from jax import lax
from jax.experimental import pallas as pl
from jax.experimental.pallas import tpu as pltpu
from jax.sharding import PartitionSpec as P

MESH = pl.DeviceIdType.MESH
AXIS = "tp"


def gathered(n):
    return n - 1 - lax.rem(lax.axis_index("dp"), 2)


def half_rows(half, direction, j):
    return pl.ds(pl.multiple_of(j * 2 * half + direction * half, half), half)


def greet(me, n):
    barrier = pltpu.get_barrier_semaphore()
    for neighbour in (lax.rem(me + 1, n), lax.rem(me + n - 1, n)):
        pl.semaphore_signal(barrier, inc=1, device_id={AXIS: neighbour}, device_id_type=MESH)
    return barrier


def kernel(
    n, x_hbm, wg_hbm, wu_hbm, wd_hbm, y, xv, wg, wu, wd, hidden, x_sem, up_sem, down_sem, send_sem, recv_sem
):
    me = lax.axis_index(AXIS)
    right, left = lax.rem(me + 1, n), lax.rem(me + n - 1, n)
    half = xv.shape[0] // 2
    up_tiles, _, up_tile = wg.shape
    down_tiles, _, down_tile = wd.shape

    def shard(direction, step):
        if direction == 0:
            return lax.rem(me + 2 * n - 1 - step, n)
        return lax.rem(me + 1 + step, n)

    def rows(direction, j):
        return half_rows(half, direction, j)

    def x_copy(direction, step):
        return pltpu.make_async_copy(
            x_hbm.at[rows(direction, shard(direction, step)), :],
            xv.at[pl.ds(direction * half, half), :],
            x_sem.at[direction],
        )

    def up_copies(t):
        columns = pl.ds(pl.multiple_of(t * up_tile, up_tile), up_tile)
        return [
            pltpu.make_async_copy(hbm.at[:, columns], vmem.at[t], up_sem.at[k, t])
            for k, (hbm, vmem) in enumerate(((wg_hbm, wg), (wu_hbm, wu)))
        ]

    def down_copy(t):
        columns = pl.ds(pl.multiple_of(t * down_tile, down_tile), down_tile)
        return pltpu.make_async_copy(wd_hbm.at[:, columns], wd.at[t], down_sem.at[t])

    def hop(direction, j, t, count):
        block = y.at[rows(direction, j), pl.ds(pl.multiple_of(t * down_tile, down_tile), down_tile)]
        return pltpu.make_async_remote_copy(
            src_ref=block,
            dst_ref=block,
            send_sem=send_sem.at[direction, t],
            recv_sem=recv_sem.at[direction, lax.rem(count, 2), t],
            device_id={AXIS: right if direction == 0 else left},
            device_id_type=MESH,
        )

    def project_up(first):
        def tile(t, _):
            if first:
                for copy in up_copies(t):
                    copy.wait()
            gate = jnp.dot(xv[...], wg[t], preferred_element_type=jnp.float32)
            up = jnp.dot(xv[...], wu[t], preferred_element_type=jnp.float32)
            columns = pl.ds(pl.multiple_of(t * up_tile, up_tile), up_tile)
            hidden[:, columns] = (jax.nn.silu(gate) * up).astype(hidden.dtype)
            return 0

        lax.fori_loop(0, up_tiles, tile, 0)

    def project_down(first, step):
        js = [shard(d, step) for d in (0, 1)]
        before = [shard(d, step - 1) for d in (0, 1)]

        def tile(t, _):
            if first:
                down_copy(t).wait()
            term = jnp.dot(hidden[...], wd[t], preferred_element_type=jnp.float32)
            columns = pl.ds(pl.multiple_of(t * down_tile, down_tile), down_tile)
            if not first:
                for d in (0, 1):
                    hop(d, js[d], t, step - 1).wait_recv()
                    hop(d, before[d], t, step - 1).wait_send()
            for d in (0, 1):
                total = term[d * half : (d + 1) * half, :]
                if not first:
                    total = total + y[rows(d, js[d]), columns].astype(jnp.float32)
                y[rows(d, js[d]), columns] = total.astype(y.dtype)

            @pl.when(t > 0)
            def _():
                for d in (0, 1):
                    hop(d, js[d], t - 1, step).start()

            return 0

        lax.fori_loop(0, down_tiles, tile, 0)
        for d in (0, 1):
            hop(d, js[d], down_tiles - 1, step).start()

    barrier = greet(me, n)

    for d in (0, 1):
        x_copy(d, 0).start()

    def start_up(t, _):
        for copy in up_copies(t):
            copy.start()
        return 0

    lax.fori_loop(0, up_tiles, start_up, 0)

    def start_down(t, _):
        down_copy(t).start()
        return 0

    lax.fori_loop(0, down_tiles, start_down, 0)

    for d in (0, 1):
        x_copy(d, 0).wait()
    project_up(True)
    for d in (0, 1):
        x_copy(d, 1).start()
    pl.semaphore_wait(barrier, 2)
    project_down(True, 0)

    def reduce_step(step, _):
        for d in (0, 1):
            x_copy(d, step).wait()
        project_up(False)

        @pl.when(step < n - 1)
        def _():
            for d in (0, 1):
                x_copy(d, step + 1).start()

        project_down(False, step)
        return 0

    lax.fori_loop(1, n, reduce_step, 0)

    last = gathered(n)

    def gather_step(step, _):
        js = [lax.rem(me + n - step, n), lax.rem(me + step, n)]
        before = [lax.rem(me + n - step + 1, n), lax.rem(me + step - 1, n)]

        def tile(t, _):
            for d in (0, 1):
                hop(d, js[d], t, n - 2 + step).wait_recv()
                hop(d, before[d], t, n - 2 + step).wait_send()

            @pl.when(step < last)
            def _():
                for d in (0, 1):
                    hop(d, js[d], t, n - 1 + step).start()

            return 0

        return lax.fori_loop(0, down_tiles, tile, 0)

    lax.fori_loop(1, last + 1, gather_step, 0)


def write_gathered(n, y, out, sem):
    me = lax.axis_index(AXIS)
    last = gathered(n)
    half = y.shape[0] // (2 * n)

    def each(act):
        def step(a, _):
            for d, j in enumerate((lax.rem(me + n - a, n), lax.rem(me + a, n))):
                block = half_rows(half, d, j)
                act(pltpu.make_async_copy(y.at[block, :], out.at[block, :], sem.at[d, a]))
            return 0

        lax.fori_loop(0, last + 1, step, 0)

    each(lambda copy: copy.start())
    each(lambda copy: copy.wait())


def last_hop(n, y, _, held, send_sem, recv_sem):
    me = lax.axis_index(AXIS)
    half = held.shape[1]
    neighbours = (lax.rem(me + 1, n), lax.rem(me + n - 1, n))
    js = (lax.rem(me + 2, n), lax.rem(me + n - 2, n))

    @pl.when(gathered(n) < n - 1)
    def _():
        barrier = greet(me, n)
        pl.semaphore_wait(barrier, 2)
        hops = [
            pltpu.make_async_remote_copy(
                src_ref=y.at[half_rows(half, d, js[d]), :],
                dst_ref=held.at[d],
                send_sem=send_sem.at[d],
                recv_sem=recv_sem.at[d],
                device_id={AXIS: neighbours[d]},
                device_id_type=MESH,
            )
            for d in (0, 1)
        ]
        for hop in hops:
            hop.start()
        for hop in hops:
            hop.wait()


def write_last(n, held, _, out, sem):
    me = lax.axis_index(AXIS)
    half = held.shape[1]
    js = (lax.rem(me + 1, n), lax.rem(me + n - 1, n))

    @pl.when(gathered(n) < n - 1)
    def _():
        copies = [
            pltpu.make_async_copy(held.at[d], out.at[half_rows(half, d, js[d]), :], sem.at[d]) for d in (0, 1)
        ]
        for copy in copies:
            copy.start()
        for copy in copies:
            copy.wait()


def solution(mesh):
    n = mesh.shape[AXIS]

    def step(x, w_gate, w_up, w_down):
        tokens, d_model = x.shape
        hidden = w_gate.shape[1]
        block = tokens // n
        up_tile, down_tile = 256, 512
        up_tiles, down_tiles = hidden // up_tile, d_model // down_tile
        y = pl.pallas_call(
            functools.partial(kernel, n),
            out_shape=pltpu.VMEM((tokens, d_model), jnp.bfloat16),
            in_specs=[pl.BlockSpec(memory_space=pl.ANY)] * 4,
            out_specs=pl.BlockSpec(memory_space=pltpu.VMEM),
            scratch_shapes=[
                pltpu.VMEM((block, d_model), jnp.bfloat16),
                pltpu.VMEM((up_tiles, d_model, up_tile), jnp.bfloat16),
                pltpu.VMEM((up_tiles, d_model, up_tile), jnp.bfloat16),
                pltpu.VMEM((down_tiles, hidden, down_tile), jnp.bfloat16),
                pltpu.VMEM((block, hidden), jnp.bfloat16),
                pltpu.SemaphoreType.DMA((2,)),
                pltpu.SemaphoreType.DMA((2, up_tiles)),
                pltpu.SemaphoreType.DMA((down_tiles,)),
                pltpu.SemaphoreType.DMA((2, down_tiles)),
                pltpu.SemaphoreType.DMA((2, 2, down_tiles)),
            ],
            compiler_params=pltpu.CompilerParams(
                collective_id=0, has_side_effects=True, vmem_limit_bytes=47 << 20
            ),
            name="mlp_ring",
        )(x, w_gate, w_up, w_down)
        in_vmem, anywhere = pl.BlockSpec(memory_space=pltpu.VMEM), pl.BlockSpec(memory_space=pl.ANY)
        y = pltpu.with_memory_space_constraint(y, pltpu.VMEM)
        whole = jax.ShapeDtypeStruct((tokens, d_model), jnp.bfloat16)
        out = pl.pallas_call(
            functools.partial(write_gathered, n),
            out_shape=whole,
            in_specs=[in_vmem],
            out_specs=anywhere,
            scratch_shapes=[pltpu.SemaphoreType.DMA((2, n))],
            compiler_params=pltpu.CompilerParams(vmem_limit_bytes=1 << 20),
            name="write_gathered",
        )(y)
        held = pl.pallas_call(
            functools.partial(last_hop, n),
            out_shape=pltpu.VMEM((2, block // 2, d_model), jnp.bfloat16),
            in_specs=[in_vmem, pl.BlockSpec(memory_space=pltpu.HBM)],
            out_specs=in_vmem,
            scratch_shapes=[pltpu.SemaphoreType.DMA((2,)), pltpu.SemaphoreType.DMA((2,))],
            compiler_params=pltpu.CompilerParams(collective_id=1, has_side_effects=True, vmem_limit_bytes=1 << 20),
            name="last_hop",
        )(y, pltpu.with_memory_space_constraint(out, pltpu.HBM))
        return pl.pallas_call(
            functools.partial(write_last, n),
            out_shape=whole,
            in_specs=[in_vmem, anywhere],
            out_specs=anywhere,
            scratch_shapes=[pltpu.SemaphoreType.DMA((2,))],
            input_output_aliases={1: 0},
            compiler_params=pltpu.CompilerParams(vmem_limit_bytes=1 << 20),
            name="write_last",
        )(pltpu.with_memory_space_constraint(held, pltpu.VMEM), out)

    return jax.shard_map(
        step,
        mesh=mesh,
        in_specs=(P("dp", None), P(None, AXIS), P(None, AXIS), P(AXIS, None)),
        out_specs=P("dp", None),
        check_vma=False,
    )
```

```python
import functools

import jax
import jax.numpy as jnp
from jax import lax
from jax.experimental import pallas as pl
from jax.experimental.pallas import tpu as pltpu
from jax.sharding import PartitionSpec as P

MESH = pl.DeviceIdType.MESH
AXIS = "tp"


def gathered(n):
    return n - 1 - lax.rem(lax.axis_index("dp"), 2)


def half_rows(half, direction, j):
    return pl.ds(pl.multiple_of(j * 2 * half + direction * half, half), half)


def greet(me, n):
    barrier = pltpu.get_barrier_semaphore()
    for neighbour in (lax.rem(me + 1, n), lax.rem(me + n - 1, n)):
        pl.semaphore_signal(barrier, inc=1, device_id={AXIS: neighbour}, device_id_type=MESH)
    return barrier


def kernel(
    n, x_hbm, wg_hbm, wu_hbm, wd_hbm, y, xv, wg, wu, wd, hidden, x_sem, up_sem, down_sem, send_sem, recv_sem
):
    me = lax.axis_index(AXIS)
    right, left = lax.rem(me + 1, n), lax.rem(me + n - 1, n)
    half = xv.shape[0] // 2
    part = half // 2
    up_tiles, _, up_tile = wg.shape
    down_tiles, _, down_tile = wd.shape

    def shard(direction, step):
        if direction == 0:
            return lax.rem(me + 2 * n - 1 - step, n)
        return lax.rem(me + 1 + step, n)

    def part_rows(direction, j, p):
        return pl.ds(pl.multiple_of(j * 2 * half + direction * half + p * part, part), part)

    def tile_columns(t, size):
        return pl.ds(pl.multiple_of(t * size, size), size)

    def x_copies(step, p):
        return [
            pltpu.make_async_copy(
                x_hbm.at[part_rows(d, shard(d, step), p), :],
                xv.at[pl.ds((2 * p + d) * part, part), :],
                x_sem.at[d, p],
            )
            for d in (0, 1)
        ]

    def up_copies(t):
        return [
            pltpu.make_async_copy(hbm.at[:, tile_columns(t, up_tile)], vmem.at[t], up_sem.at[k, t])
            for k, (hbm, vmem) in enumerate(((wg_hbm, wg), (wu_hbm, wu)))
        ]

    def down_copy(t):
        return pltpu.make_async_copy(wd_hbm.at[:, tile_columns(t, down_tile)], wd.at[t], down_sem.at[t])

    def send(direction, block, t, count):
        return pltpu.make_async_remote_copy(
            src_ref=block,
            dst_ref=block,
            send_sem=send_sem.at[direction, t],
            recv_sem=recv_sem.at[direction, lax.rem(count, 2), t],
            device_id={AXIS: right if direction == 0 else left},
            device_id_type=MESH,
        )

    def hop(direction, j, t, count):
        return send(direction, y.at[half_rows(half, direction, j), tile_columns(t, down_tile)], t, count)

    def first_hop(direction, p, t):
        rows = part_rows(direction, shard(direction, 0), p)
        return send(direction, y.at[rows, tile_columns(t, down_tile)], t, 0)

    def project_up(rows, arriving=False, unroll=True):
        def tile(t, _):
            if arriving:
                for copy in up_copies(t):
                    copy.wait()
            gate = jnp.dot(xv[rows, :], wg[t], preferred_element_type=jnp.float32)
            up = jnp.dot(xv[rows, :], wu[t], preferred_element_type=jnp.float32)
            hidden[rows, tile_columns(t, up_tile)] = (jax.nn.silu(gate) * up).astype(hidden.dtype)
            return 0

        lax.fori_loop(0, up_tiles, tile, 0, unroll=unroll and not arriving)

    def project_first_down(p):
        rows = pl.ds(2 * p * part, 2 * part)

        def start(t):
            for d in (0, 1):
                first_hop(d, p, t).start()

        def tiles(ts):
            if p == 0:
                for t in ts:
                    down_copy(t).wait()
            for t in ts:
                term = jnp.dot(hidden[rows, :], wd[t], preferred_element_type=jnp.float32)
                for d in (0, 1):
                    y[part_rows(d, shard(d, 0), p), tile_columns(t, down_tile)] = term[
                        d * part : (d + 1) * part, :
                    ].astype(y.dtype)

        def pair(g, _):
            tiles((2 * g, 2 * g + 1))

            @pl.when(g > 1)
            def _():
                start(2 * g - 2)

            start(2 * g - 1)
            return 0

        tiles((0,))
        tiles((1,))
        start(0)
        lax.fori_loop(1, down_tiles // 2, pair, 0)
        start(down_tiles - 2)
        start(down_tiles - 1)

    def project_down(step):
        js = [shard(d, step) for d in (0, 1)]
        before = [shard(d, step - 1) for d in (0, 1)]

        def tile(t, _):
            columns = tile_columns(t, down_tile)
            term = jnp.dot(hidden[...], wd[t], preferred_element_type=jnp.float32)
            for d in (0, 1):
                hop(d, js[d], t, step - 1).wait_recv()
                hop(d, before[d], t, step - 1).wait_send()
            for d in (0, 1):
                for p in (0, 1):
                    rows = part_rows(d, js[d], p)
                    own = term[(2 * p + d) * part : (2 * p + d + 1) * part, :]
                    y[rows, columns] = (own + y[rows, columns].astype(jnp.float32)).astype(y.dtype)

            @pl.when(t > 0)
            def _():
                for d in (0, 1):
                    hop(d, js[d], t - 1, step).start()

            return 0

        lax.fori_loop(0, down_tiles, tile, 0)
        for d in (0, 1):
            hop(d, js[d], down_tiles - 1, step).start()

    barrier = greet(me, n)

    for copy in x_copies(0, 0):
        copy.start()

    def start_up(t, _):
        for copy in up_copies(t):
            copy.start()
        return 0

    lax.fori_loop(0, up_tiles, start_up, 0)

    def start_down(t, _):
        down_copy(t).start()
        return 0

    lax.fori_loop(0, down_tiles, start_down, 0)
    for copy in x_copies(0, 1):
        copy.start()

    for p in (0, 1):
        for copy in x_copies(0, p):
            copy.wait()
        project_up(pl.ds(2 * p * part, 2 * part), arriving=p == 0)
        for copy in x_copies(1, p):
            copy.start()
        if p == 0:
            pl.semaphore_wait(barrier, 2)
        project_first_down(p)

    def reduce_step(step, _):
        for p in (0, 1):
            for copy in x_copies(step, p):
                copy.wait()
        project_up(pl.ds(0, 2 * half), unroll=False)

        @pl.when(step < n - 1)
        def _():
            for p in (0, 1):
                for copy in x_copies(step + 1, p):
                    copy.start()

        project_down(step)
        return 0

    lax.fori_loop(1, n, reduce_step, 0)

    last = gathered(n)

    def gather_step(step, _):
        js = [lax.rem(me + n - step, n), lax.rem(me + step, n)]
        before = [lax.rem(me + n - step + 1, n), lax.rem(me + step - 1, n)]

        def tile(t, _):
            for d in (0, 1):
                hop(d, js[d], t, n - 2 + step).wait_recv()
                hop(d, before[d], t, n - 2 + step).wait_send()

            @pl.when(step < last)
            def _():
                for d in (0, 1):
                    hop(d, js[d], t, n - 1 + step).start()

            return 0

        return lax.fori_loop(0, down_tiles, tile, 0)

    lax.fori_loop(1, last + 1, gather_step, 0)


def write_gathered(n, y, out, sem):
    me = lax.axis_index(AXIS)
    last = gathered(n)
    half = y.shape[0] // (2 * n)

    def each(act):
        def step(a, _):
            for d, j in enumerate((lax.rem(me + n - a, n), lax.rem(me + a, n))):
                block = half_rows(half, d, j)
                act(pltpu.make_async_copy(y.at[block, :], out.at[block, :], sem.at[d, a]))
            return 0

        lax.fori_loop(0, last + 1, step, 0)

    each(lambda copy: copy.start())
    each(lambda copy: copy.wait())


def last_hop(n, y, _, held, send_sem, recv_sem):
    me = lax.axis_index(AXIS)
    half = held.shape[1]
    neighbours = (lax.rem(me + 1, n), lax.rem(me + n - 1, n))
    js = (lax.rem(me + 2, n), lax.rem(me + n - 2, n))

    @pl.when(gathered(n) < n - 1)
    def _():
        barrier = greet(me, n)
        pl.semaphore_wait(barrier, 2)
        hops = [
            pltpu.make_async_remote_copy(
                src_ref=y.at[half_rows(half, d, js[d]), :],
                dst_ref=held.at[d],
                send_sem=send_sem.at[d],
                recv_sem=recv_sem.at[d],
                device_id={AXIS: neighbours[d]},
                device_id_type=MESH,
            )
            for d in (0, 1)
        ]
        for hop in hops:
            hop.start()
        for hop in hops:
            hop.wait()


def write_last(n, held, _, out, sem):
    me = lax.axis_index(AXIS)
    half = held.shape[1]
    js = (lax.rem(me + 1, n), lax.rem(me + n - 1, n))

    @pl.when(gathered(n) < n - 1)
    def _():
        copies = [
            pltpu.make_async_copy(held.at[d], out.at[half_rows(half, d, js[d]), :], sem.at[d]) for d in (0, 1)
        ]
        for copy in copies:
            copy.start()
        for copy in copies:
            copy.wait()


def solution(mesh):
    n = mesh.shape[AXIS]

    def step(x, w_gate, w_up, w_down):
        tokens, d_model = x.shape
        hidden = w_gate.shape[1]
        block = tokens // n
        up_tile, down_tile = 256, 256
        up_tiles, down_tiles = hidden // up_tile, d_model // down_tile
        y = pl.pallas_call(
            functools.partial(kernel, n),
            out_shape=pltpu.VMEM((tokens, d_model), jnp.bfloat16),
            in_specs=[pl.BlockSpec(memory_space=pl.ANY)] * 4,
            out_specs=pl.BlockSpec(memory_space=pltpu.VMEM),
            scratch_shapes=[
                pltpu.VMEM((block, d_model), jnp.bfloat16),
                pltpu.VMEM((up_tiles, d_model, up_tile), jnp.bfloat16),
                pltpu.VMEM((up_tiles, d_model, up_tile), jnp.bfloat16),
                pltpu.VMEM((down_tiles, hidden, down_tile), jnp.bfloat16),
                pltpu.VMEM((block, hidden), jnp.bfloat16),
                pltpu.SemaphoreType.DMA((2, 2)),
                pltpu.SemaphoreType.DMA((2, up_tiles)),
                pltpu.SemaphoreType.DMA((down_tiles,)),
                pltpu.SemaphoreType.DMA((2, down_tiles)),
                pltpu.SemaphoreType.DMA((2, 2, down_tiles)),
            ],
            compiler_params=pltpu.CompilerParams(
                collective_id=0, has_side_effects=True, vmem_limit_bytes=47 << 20
            ),
            name="mlp_ring",
        )(x, w_gate, w_up, w_down)
        in_vmem, anywhere = pl.BlockSpec(memory_space=pltpu.VMEM), pl.BlockSpec(memory_space=pl.ANY)
        y = pltpu.with_memory_space_constraint(y, pltpu.VMEM)
        whole = jax.ShapeDtypeStruct((tokens, d_model), jnp.bfloat16)
        out = pl.pallas_call(
            functools.partial(write_gathered, n),
            out_shape=whole,
            in_specs=[in_vmem],
            out_specs=anywhere,
            scratch_shapes=[pltpu.SemaphoreType.DMA((2, n))],
            compiler_params=pltpu.CompilerParams(vmem_limit_bytes=1 << 20),
            name="write_gathered",
        )(y)
        held = pl.pallas_call(
            functools.partial(last_hop, n),
            out_shape=pltpu.VMEM((2, block // 2, d_model), jnp.bfloat16),
            in_specs=[in_vmem, pl.BlockSpec(memory_space=pltpu.HBM)],
            out_specs=in_vmem,
            scratch_shapes=[pltpu.SemaphoreType.DMA((2,)), pltpu.SemaphoreType.DMA((2,))],
            compiler_params=pltpu.CompilerParams(collective_id=1, has_side_effects=True, vmem_limit_bytes=1 << 20),
            name="last_hop",
        )(y, pltpu.with_memory_space_constraint(out, pltpu.HBM))
        return pl.pallas_call(
            functools.partial(write_last, n),
            out_shape=whole,
            in_specs=[in_vmem, anywhere],
            out_specs=anywhere,
            scratch_shapes=[pltpu.SemaphoreType.DMA((2,))],
            input_output_aliases={1: 0},
            compiler_params=pltpu.CompilerParams(vmem_limit_bytes=1 << 20),
            name="write_last",
        )(pltpu.with_memory_space_constraint(held, pltpu.VMEM), out)

    return jax.shard_map(
        step,
        mesh=mesh,
        in_specs=(P("dp", None), P(None, AXIS), P(None, AXIS), P(AXIS, None)),
        out_specs=P("dp", None),
        check_vma=False,
    )
```

```python
import functools

import jax
import jax.numpy as jnp
from jax import lax
from jax.experimental import pallas as pl
from jax.experimental.pallas import tpu as pltpu
from jax.sharding import PartitionSpec as P

MESH = pl.DeviceIdType.MESH
AXIS, GROUPS = "tp", "dp"


def gathered(n):
    return n - 1 - lax.rem(lax.axis_index(GROUPS), 2)


def half_rows(half, direction, j):
    return pl.ds(pl.multiple_of(j * 2 * half + direction * half, half), half)


def greet(*others):
    barrier = pltpu.get_barrier_semaphore()
    for other in others:
        pl.semaphore_signal(barrier, inc=1, device_id=other, device_id_type=MESH)
    return barrier


def kernel(
    n,
    x_hbm,
    wg_hbm,
    wu_hbm,
    wd_hbm,
    y,
    xv,
    wg,
    wu,
    wd,
    hidden,
    x_sem,
    up_sem,
    down_sem,
    send_sem,
    recv_sem,
    share_send,
    share_recv,
):
    me = lax.axis_index(AXIS)
    right, left = lax.rem(me + 1, n), lax.rem(me + n - 1, n)
    half = xv.shape[0] // 2
    part = half // 2
    up_tiles, _, up_tile = wg.shape
    down_tiles, _, down_tile = wd.shape
    group = lax.axis_index(GROUPS)
    core = lax.rem(group, 2)
    partner = {GROUPS: group + 1 - 2 * core}
    split = (up_tiles + 1) // 2
    first, stop = core * split, split + core * (up_tiles - split)
    own, other = pl.ds(0, 2 * part), pl.ds(2 * part, 2 * part)

    def shard(direction, step):
        if direction == 0:
            return lax.rem(me + 2 * n - 1 - step, n)
        return lax.rem(me + 1 + step, n)

    def part_rows(direction, j, p):
        return pl.ds(pl.multiple_of(j * 2 * half + direction * half + p * part, part), part)

    def tile_columns(t, size):
        return pl.ds(pl.multiple_of(t * size, size), size)

    def x_copies(step, p):
        return [
            pltpu.make_async_copy(
                x_hbm.at[part_rows(d, shard(d, step), p), :],
                xv.at[pl.ds((2 * p + d) * part, part), :],
                x_sem.at[d, p],
            )
            for d in (0, 1)
        ]

    def up_copies(t):
        return [
            pltpu.make_async_copy(hbm.at[:, tile_columns(t, up_tile)], vmem.at[t], up_sem.at[k, t])
            for k, (hbm, vmem) in enumerate(((wg_hbm, wg), (wu_hbm, wu)))
        ]

    def down_copy(t):
        return pltpu.make_async_copy(wd_hbm.at[:, tile_columns(t, down_tile)], wd.at[t], down_sem.at[t])

    def send(direction, block, t, count):
        return pltpu.make_async_remote_copy(
            src_ref=block,
            dst_ref=block,
            send_sem=send_sem.at[direction, t],
            recv_sem=recv_sem.at[direction, lax.rem(count, 2), t],
            device_id={AXIS: right if direction == 0 else left},
            device_id_type=MESH,
        )

    def hop(direction, j, t, count):
        return send(direction, y.at[half_rows(half, direction, j), tile_columns(t, down_tile)], t, count)

    def first_hop(direction, p, t):
        rows = part_rows(direction, shard(direction, 0), p)
        return send(direction, y.at[rows, tile_columns(t, down_tile)], t, 0)

    def each_tile(low, high, act):
        def tile(t, _):
            act(t)
            return 0

        lax.fori_loop(low, high, tile, 0)

    def each_other_tile(act):
        each_tile(0, first, act)
        each_tile(stop, up_tiles, act)

    def start_up(t):
        for copy in up_copies(t):
            copy.start()

    def wait_up(t):
        for copy in up_copies(t):
            copy.wait()

    def share(src, dst, k):
        return pltpu.make_async_remote_copy(
            src_ref=src,
            dst_ref=dst,
            send_sem=share_send.at[k],
            recv_sem=share_recv.at[k],
            device_id=partner,
            device_id_type=MESH,
        )

    def share_x():
        return share(xv.at[own, :], xv.at[other, :], up_tiles)

    def share_hidden(t):
        columns = tile_columns(t, up_tile)
        return share(hidden.at[other, columns], hidden.at[own, columns], t)

    def up_tile_of(rows, t):
        gate = jnp.dot(xv[rows, :], wg[t], preferred_element_type=jnp.float32)
        up = jnp.dot(xv[rows, :], wu[t], preferred_element_type=jnp.float32)
        hidden[rows, tile_columns(t, up_tile)] = (jax.nn.silu(gate) * up).astype(hidden.dtype)

    def project_up():
        each_tile(0, up_tiles, lambda t: up_tile_of(pl.ds(0, 2 * half), t))

    def project_second_up():
        order = [lax.rem(first + k, up_tiles) for k in range(up_tiles)]
        present = up_tiles - split
        for t in order[:present]:
            up_tile_of(other, t)
        each_other_tile(wait_up)
        for t in order[present:]:
            up_tile_of(other, t)

    def project_shared():
        wait_up(first)
        up_tile_of(own, first)
        share_x().wait_recv()
        up_tile_of(other, first)

        def tile(t, _):
            wait_up(t)
            up_tile_of(pl.ds(0, 2 * half), t)
            share_hidden(t - 1).start()
            return 0

        lax.fori_loop(first + 1, stop, tile, 0)
        share_hidden(stop - 1).start()

    def project_first_down(p):
        rows = pl.ds(2 * p * part, 2 * part)

        def start(t):
            for d in (0, 1):
                first_hop(d, p, t).start()

        def tiles(ts):
            if p == 0:
                for t in ts:
                    down_copy(t).wait()
            for t in ts:
                term = jnp.dot(hidden[rows, :], wd[t], preferred_element_type=jnp.float32)
                for d in (0, 1):
                    y[part_rows(d, shard(d, 0), p), tile_columns(t, down_tile)] = term[
                        d * part : (d + 1) * part, :
                    ].astype(y.dtype)

        def pair(g, _):
            tiles((2 * g, 2 * g + 1))

            @pl.when(g > 1)
            def _():
                start(2 * g - 2)

            start(2 * g - 1)
            return 0

        tiles((0,))
        tiles((1,))
        start(0)
        lax.fori_loop(1, down_tiles // 2, pair, 0)
        start(down_tiles - 2)
        start(down_tiles - 1)

    def project_down(step):
        js = [shard(d, step) for d in (0, 1)]
        before = [shard(d, step - 1) for d in (0, 1)]

        def tile(t, _):
            columns = tile_columns(t, down_tile)
            term = jnp.dot(hidden[...], wd[t], preferred_element_type=jnp.float32)
            for d in (0, 1):
                hop(d, js[d], t, step - 1).wait_recv()
                hop(d, before[d], t, step - 1).wait_send()
            for d in (0, 1):
                for p in (0, 1):
                    rows = part_rows(d, js[d], p)
                    own = term[(2 * p + d) * part : (2 * p + d + 1) * part, :]
                    y[rows, columns] = (own + y[rows, columns].astype(jnp.float32)).astype(y.dtype)

            @pl.when(t > 0)
            def _():
                for d in (0, 1):
                    hop(d, js[d], t - 1, step).start()

            return 0

        lax.fori_loop(0, down_tiles, tile, 0)
        for d in (0, 1):
            hop(d, js[d], down_tiles - 1, step).start()

    barrier = greet({AXIS: left}, {AXIS: right}, partner)

    for copy in x_copies(0, 0):
        copy.start()
    each_tile(first, stop, start_up)
    each_tile(0, down_tiles, lambda t: down_copy(t).start())

    for copy in x_copies(0, 0):
        copy.wait()
    pl.semaphore_wait(barrier, 3)
    share_x().start()
    project_shared()
    for copy in x_copies(0, 1):
        copy.start()
    each_other_tile(start_up)
    each_other_tile(lambda t: share_hidden(t).wait_recv())
    project_first_down(0)

    for copy in x_copies(0, 1):
        copy.wait()
    share_x().wait_send()
    each_tile(first, stop, lambda t: share_hidden(t).wait_send())
    for copy in x_copies(1, 0):
        copy.start()
    project_second_up()
    for copy in x_copies(1, 1):
        copy.start()
    project_first_down(1)

    def reduce_step(step, _):
        for p in (0, 1):
            for copy in x_copies(step, p):
                copy.wait()
        project_up()

        @pl.when(step < n - 1)
        def _():
            for p in (0, 1):
                for copy in x_copies(step + 1, p):
                    copy.start()

        project_down(step)
        return 0

    lax.fori_loop(1, n, reduce_step, 0)

    last = gathered(n)

    def gather_step(step, _):
        js = [lax.rem(me + n - step, n), lax.rem(me + step, n)]
        before = [lax.rem(me + n - step + 1, n), lax.rem(me + step - 1, n)]

        def tile(t, _):
            for d in (0, 1):
                hop(d, js[d], t, n - 2 + step).wait_recv()
                hop(d, before[d], t, n - 2 + step).wait_send()

            @pl.when(step < last)
            def _():
                for d in (0, 1):
                    hop(d, js[d], t, n - 1 + step).start()

            return 0

        return lax.fori_loop(0, down_tiles, tile, 0)

    lax.fori_loop(1, last + 1, gather_step, 0)


def write_gathered(n, y, out, sem):
    me = lax.axis_index(AXIS)
    last = gathered(n)
    half = y.shape[0] // (2 * n)

    def each(act):
        def step(a, _):
            for d, j in enumerate((lax.rem(me + n - a, n), lax.rem(me + a, n))):
                block = half_rows(half, d, j)
                act(pltpu.make_async_copy(y.at[block, :], out.at[block, :], sem.at[d, a]))
            return 0

        lax.fori_loop(0, last + 1, step, 0)

    each(lambda copy: copy.start())
    each(lambda copy: copy.wait())


def last_hop(n, y, _, held, send_sem, recv_sem):
    me = lax.axis_index(AXIS)
    half = held.shape[1]
    neighbours = (lax.rem(me + 1, n), lax.rem(me + n - 1, n))
    js = (lax.rem(me + 2, n), lax.rem(me + n - 2, n))

    @pl.when(gathered(n) < n - 1)
    def _():
        barrier = greet({AXIS: neighbours[0]}, {AXIS: neighbours[1]})
        pl.semaphore_wait(barrier, 2)
        hops = [
            pltpu.make_async_remote_copy(
                src_ref=y.at[half_rows(half, d, js[d]), :],
                dst_ref=held.at[d],
                send_sem=send_sem.at[d],
                recv_sem=recv_sem.at[d],
                device_id={AXIS: neighbours[d]},
                device_id_type=MESH,
            )
            for d in (0, 1)
        ]
        for hop in hops:
            hop.start()
        for hop in hops:
            hop.wait()


def write_last(n, held, _, out, sem):
    me = lax.axis_index(AXIS)
    half = held.shape[1]
    js = (lax.rem(me + 1, n), lax.rem(me + n - 1, n))

    @pl.when(gathered(n) < n - 1)
    def _():
        copies = [
            pltpu.make_async_copy(held.at[d], out.at[half_rows(half, d, js[d]), :], sem.at[d]) for d in (0, 1)
        ]
        for copy in copies:
            copy.start()
        for copy in copies:
            copy.wait()


def solution(mesh):
    n = mesh.shape[AXIS]

    def step(x, w_gate, w_up, w_down):
        tokens, d_model = x.shape
        hidden = w_gate.shape[1]
        block = tokens // n
        up_tile, down_tile = 256, 256
        up_tiles, down_tiles = hidden // up_tile, d_model // down_tile
        y = pl.pallas_call(
            functools.partial(kernel, n),
            out_shape=pltpu.VMEM((tokens, d_model), jnp.bfloat16),
            in_specs=[pl.BlockSpec(memory_space=pl.ANY)] * 4,
            out_specs=pl.BlockSpec(memory_space=pltpu.VMEM),
            scratch_shapes=[
                pltpu.VMEM((block, d_model), jnp.bfloat16),
                pltpu.VMEM((up_tiles, d_model, up_tile), jnp.bfloat16),
                pltpu.VMEM((up_tiles, d_model, up_tile), jnp.bfloat16),
                pltpu.VMEM((down_tiles, hidden, down_tile), jnp.bfloat16),
                pltpu.VMEM((block, hidden), jnp.bfloat16),
                pltpu.SemaphoreType.DMA((2, 2)),
                pltpu.SemaphoreType.DMA((2, up_tiles)),
                pltpu.SemaphoreType.DMA((down_tiles,)),
                pltpu.SemaphoreType.DMA((2, down_tiles)),
                pltpu.SemaphoreType.DMA((2, 2, down_tiles)),
                pltpu.SemaphoreType.DMA((up_tiles + 1,)),
                pltpu.SemaphoreType.DMA((up_tiles + 1,)),
            ],
            compiler_params=pltpu.CompilerParams(
                collective_id=0, has_side_effects=True, vmem_limit_bytes=50_200_000
            ),
            name="mlp_ring",
        )(x, w_gate, w_up, w_down)
        in_vmem, anywhere = pl.BlockSpec(memory_space=pltpu.VMEM), pl.BlockSpec(memory_space=pl.ANY)
        y = pltpu.with_memory_space_constraint(y, pltpu.VMEM)
        whole = jax.ShapeDtypeStruct((tokens, d_model), jnp.bfloat16)
        out = pl.pallas_call(
            functools.partial(write_gathered, n),
            out_shape=whole,
            in_specs=[in_vmem],
            out_specs=anywhere,
            scratch_shapes=[pltpu.SemaphoreType.DMA((2, n))],
            compiler_params=pltpu.CompilerParams(vmem_limit_bytes=1 << 20),
            name="write_gathered",
        )(y)
        held = pl.pallas_call(
            functools.partial(last_hop, n),
            out_shape=pltpu.VMEM((2, block // 2, d_model), jnp.bfloat16),
            in_specs=[in_vmem, pl.BlockSpec(memory_space=pltpu.HBM)],
            out_specs=in_vmem,
            scratch_shapes=[pltpu.SemaphoreType.DMA((2,)), pltpu.SemaphoreType.DMA((2,))],
            compiler_params=pltpu.CompilerParams(collective_id=1, has_side_effects=True, vmem_limit_bytes=1 << 20),
            name="last_hop",
        )(y, pltpu.with_memory_space_constraint(out, pltpu.HBM))
        return pl.pallas_call(
            functools.partial(write_last, n),
            out_shape=whole,
            in_specs=[in_vmem, anywhere],
            out_specs=anywhere,
            scratch_shapes=[pltpu.SemaphoreType.DMA((2,))],
            input_output_aliases={1: 0},
            compiler_params=pltpu.CompilerParams(vmem_limit_bytes=1 << 20),
            name="write_last",
        )(pltpu.with_memory_space_constraint(held, pltpu.VMEM), out)

    return jax.shard_map(
        step,
        mesh=mesh,
        in_specs=(P("dp", None), P(None, AXIS), P(None, AXIS), P(AXIS, None)),
        out_specs=P("dp", None),
        check_vma=False,
    )
```

```python
import functools

import jax
import jax.numpy as jnp
from jax import lax
from jax.experimental import pallas as pl
from jax.experimental.pallas import tpu as pltpu
from jax.sharding import PartitionSpec as P

MESH = pl.DeviceIdType.MESH
AXIS, GROUPS = "tp", "dp"


def gathered(n):
    return n - 2 + lax.rem(lax.axis_index(GROUPS), 2)


def half_rows(half, direction, j):
    return pl.ds(pl.multiple_of(j * 2 * half + direction * half, half), half)


def greet(*others):
    barrier = pltpu.get_barrier_semaphore()
    for other in others:
        pl.semaphore_signal(barrier, inc=1, device_id=other, device_id_type=MESH)
    return barrier


def kernel(
    n,
    x_hbm,
    wg_hbm,
    wu_hbm,
    wd_hbm,
    y,
    xv,
    wg,
    wu,
    wd,
    hidden,
    x_sem,
    up_sem,
    down_sem,
    send_sem,
    recv_sem,
    share_send,
    share_recv,
    told,
):
    me = lax.axis_index(AXIS)
    right, left = lax.rem(me + 1, n), lax.rem(me + n - 1, n)
    half = xv.shape[0] // 2
    part = half // 2
    up_tiles, _, up_tile = wg.shape
    down_tiles, _, down_tile = wd.shape
    group = lax.axis_index(GROUPS)
    core = lax.rem(group, 2)
    partner = {GROUPS: group + 1 - 2 * core}
    shared = up_tiles // 2
    first, theirs = core * (up_tiles - shared), (1 - core) * (up_tiles - shared)
    between = range(shared, up_tiles - shared)
    own, other = pl.ds(0, 2 * part), pl.ds(2 * part, 2 * part)

    def shard(direction, step):
        if direction == 0:
            return lax.rem(me + 2 * n - 1 - step, n)
        return lax.rem(me + 1 + step, n)

    def part_rows(direction, j, p):
        return pl.ds(pl.multiple_of(j * 2 * half + direction * half + p * part, part), part)

    def tile_columns(t, size):
        return pl.ds(pl.multiple_of(t * size, size), size)

    def x_copies(step, p):
        return [
            pltpu.make_async_copy(
                x_hbm.at[part_rows(d, shard(d, step), p), :],
                xv.at[pl.ds((2 * p + d) * part, part), :],
                x_sem.at[d, p],
            )
            for d in (0, 1)
        ]

    def up_copies(t):
        return [
            pltpu.make_async_copy(hbm.at[:, tile_columns(t, up_tile)], vmem.at[t], up_sem.at[k, t])
            for k, (hbm, vmem) in enumerate(((wg_hbm, wg), (wu_hbm, wu)))
        ]

    def down_copy(t):
        return pltpu.make_async_copy(wd_hbm.at[:, tile_columns(t, down_tile)], wd.at[t], down_sem.at[t])

    def send(direction, block, t, count):
        return pltpu.make_async_remote_copy(
            src_ref=block,
            dst_ref=block,
            send_sem=send_sem.at[direction, t],
            recv_sem=recv_sem.at[direction, lax.rem(count, 2), t],
            device_id={AXIS: right if direction == 0 else left},
            device_id_type=MESH,
        )

    def hop(direction, j, t, count):
        return send(direction, y.at[half_rows(half, direction, j), tile_columns(t, down_tile)], t, count)

    def first_hop(direction, p, t):
        rows = part_rows(direction, shard(direction, 0), p)
        return send(direction, y.at[rows, tile_columns(t, down_tile)], t, 0)

    def each_tile(low, high, act):
        def tile(t, _):
            act(t)
            return 0

        lax.fori_loop(low, high, tile, 0)

    def start_up(t):
        for copy in up_copies(t):
            copy.start()

    def wait_up(t):
        for copy in up_copies(t):
            copy.wait()

    def share(src, dst, k):
        return pltpu.make_async_remote_copy(
            src_ref=src,
            dst_ref=dst,
            send_sem=share_send.at[k],
            recv_sem=share_recv.at[k],
            device_id=partner,
            device_id_type=MESH,
        )

    def share_x():
        return share(xv.at[own, :], xv.at[other, :], up_tiles)

    def share_hidden(t):
        columns = tile_columns(t, up_tile)
        return share(hidden.at[other, columns], hidden.at[own, columns], t)

    def up_tile_of(rows, t):
        gate = jnp.dot(xv[rows, :], wg[t], preferred_element_type=jnp.float32)
        up = jnp.dot(xv[rows, :], wu[t], preferred_element_type=jnp.float32)
        hidden[rows, tile_columns(t, up_tile)] = (jax.nn.silu(gate) * up).astype(hidden.dtype)

    def project_up():
        each_tile(0, up_tiles, lambda t: up_tile_of(pl.ds(0, 2 * half), t))

    def project_second_up():
        for t in [first + k for k in range(shared)] + list(between):
            up_tile_of(other, t)
        each_tile(theirs, theirs + shared, wait_up)
        each_tile(theirs, theirs + shared, lambda t: up_tile_of(other, t))

    def project_shared():
        last = first + shared - 1
        wait_up(first)
        up_tile_of(own, first)
        share_x().wait_recv()
        up_tile_of(other, first)

        def tile(t, _):
            wait_up(t)
            up_tile_of(pl.ds(0, 2 * half), t)
            share_hidden(t - 1).start()
            return 0

        lax.fori_loop(first + 1, last, tile, 0)
        wait_up(last)
        up_tile_of(other, last)
        for t in (last - 1, last):
            share_hidden(t).start()

        @pl.when(core == 1)
        def _():
            pl.semaphore_wait(barrier, 4)
            pl.semaphore_signal(told, inc=1, device_id=partner, device_id_type=MESH)

        up_tile_of(own, last)
        for t in between:
            wait_up(t)
            up_tile_of(own, t)

    def project_first_down(p):
        rows = pl.ds(2 * p * part, 2 * part)
        singles = 4 if p == 0 else 2

        def start(t):
            for d in (0, 1):
                first_hop(d, p, t).start()

        def tiles(ts):
            if p == 0:
                for t in ts:
                    down_copy(t).wait()
            for t in ts:
                term = jnp.dot(hidden[rows, :], wd[t], preferred_element_type=jnp.float32)
                for d in (0, 1):
                    y[part_rows(d, shard(d, 0), p), tile_columns(t, down_tile)] = term[
                        d * part : (d + 1) * part, :
                    ].astype(y.dtype)

        def single(t, _):
            tiles((t,))
            start(t - 1)
            return 0

        def pair(g, _):
            tiles((2 * g, 2 * g + 1))

            @pl.when(2 * g > singles)
            def _():
                start(2 * g - 2)

            start(2 * g - 1)
            return 0

        tiles((0,))
        lax.fori_loop(1, singles, single, 0)
        lax.fori_loop(singles // 2, down_tiles // 2, pair, 0)
        start(down_tiles - 2)
        start(down_tiles - 1)

    def project_down(step):
        js = [shard(d, step) for d in (0, 1)]
        before = [shard(d, step - 1) for d in (0, 1)]

        def tile(t, _):
            columns = tile_columns(t, down_tile)
            term = jnp.dot(hidden[...], wd[t], preferred_element_type=jnp.float32)
            for d in (0, 1):
                hop(d, js[d], t, step - 1).wait_recv()
                hop(d, before[d], t, step - 1).wait_send()
            for d in (0, 1):
                for p in (0, 1):
                    rows = part_rows(d, js[d], p)
                    own = term[(2 * p + d) * part : (2 * p + d + 1) * part, :]
                    y[rows, columns] = (own + y[rows, columns].astype(jnp.float32)).astype(y.dtype)

            @pl.when(t > 0)
            def _():
                for d in (0, 1):
                    hop(d, js[d], t - 1, step).start()

            return 0

        lax.fori_loop(0, down_tiles, tile, 0)
        for d in (0, 1):
            hop(d, js[d], down_tiles - 1, step).start()

    listener = group - core + 1
    barrier = greet({AXIS: left, GROUPS: listener}, {AXIS: right, GROUPS: listener})

    @pl.when(core == 1)
    def _():
        pl.semaphore_signal(barrier, inc=1, device_id=partner, device_id_type=MESH)

    for copy in x_copies(0, 0):
        copy.start()
    each_tile(first, first + shared, start_up)
    for t in between:
        start_up(t)
    each_tile(0, down_tiles, lambda t: down_copy(t).start())

    @pl.when(core == 0)
    def _():
        pl.semaphore_wait(barrier, 1)
        pl.semaphore_signal(told, inc=1, device_id=partner, device_id_type=MESH)

    @pl.when(core == 1)
    def _():
        pl.semaphore_wait(told, 1)

    for copy in x_copies(0, 0):
        copy.wait()
    share_x().start()
    project_shared()

    @pl.when(core == 0)
    def _():
        pl.semaphore_wait(told, 1)

    for copy in x_copies(0, 1):
        copy.start()
    each_tile(theirs, theirs + shared, start_up)
    each_tile(theirs, theirs + shared, lambda t: share_hidden(t).wait_recv())
    project_first_down(0)

    for copy in x_copies(0, 1):
        copy.wait()
    share_x().wait_send()
    each_tile(first, first + shared, lambda t: share_hidden(t).wait_send())
    for copy in x_copies(1, 0):
        copy.start()
    project_second_up()
    for copy in x_copies(1, 1):
        copy.start()
    project_first_down(1)

    def reduce_step(step, _):
        for p in (0, 1):
            for copy in x_copies(step, p):
                copy.wait()
        project_up()

        @pl.when(step < n - 1)
        def _():
            for p in (0, 1):
                for copy in x_copies(step + 1, p):
                    copy.start()

        project_down(step)
        return 0

    lax.fori_loop(1, n, reduce_step, 0)

    last = gathered(n)

    def gather_step(step, _):
        js = [lax.rem(me + n - step, n), lax.rem(me + step, n)]
        before = [lax.rem(me + n - step + 1, n), lax.rem(me + step - 1, n)]

        def tile(t, _):
            for d in (0, 1):
                hop(d, js[d], t, n - 2 + step).wait_recv()
                hop(d, before[d], t, n - 2 + step).wait_send()

            @pl.when(step < last)
            def _():
                for d in (0, 1):
                    hop(d, js[d], t, n - 1 + step).start()

            return 0

        return lax.fori_loop(0, down_tiles, tile, 0)

    lax.fori_loop(1, last + 1, gather_step, 0)


def write_gathered(n, y, out, sem):
    me = lax.axis_index(AXIS)
    last = gathered(n)
    half = y.shape[0] // (2 * n)

    def each(act):
        def step(a, _):
            for d, j in enumerate((lax.rem(me + n - a, n), lax.rem(me + a, n))):
                block = half_rows(half, d, j)
                act(pltpu.make_async_copy(y.at[block, :], out.at[block, :], sem.at[d, a]))
            return 0

        lax.fori_loop(0, last + 1, step, 0)

    each(lambda copy: copy.start())
    each(lambda copy: copy.wait())


def last_hop(n, y, _, held, send_sem, recv_sem):
    me = lax.axis_index(AXIS)
    half = held.shape[1]
    neighbours = (lax.rem(me + 1, n), lax.rem(me + n - 1, n))
    js = (lax.rem(me + 2, n), lax.rem(me + n - 2, n))

    @pl.when(gathered(n) < n - 1)
    def _():
        barrier = greet({AXIS: neighbours[0]}, {AXIS: neighbours[1]})
        pl.semaphore_wait(barrier, 2)
        hops = [
            pltpu.make_async_remote_copy(
                src_ref=y.at[half_rows(half, d, js[d]), :],
                dst_ref=held.at[d],
                send_sem=send_sem.at[d],
                recv_sem=recv_sem.at[d],
                device_id={AXIS: neighbours[d]},
                device_id_type=MESH,
            )
            for d in (0, 1)
        ]
        for hop in hops:
            hop.start()
        for hop in hops:
            hop.wait()


def write_last(n, held, _, out, sem):
    me = lax.axis_index(AXIS)
    half = held.shape[1]
    js = (lax.rem(me + 1, n), lax.rem(me + n - 1, n))

    @pl.when(gathered(n) < n - 1)
    def _():
        copies = [
            pltpu.make_async_copy(held.at[d], out.at[half_rows(half, d, js[d]), :], sem.at[d]) for d in (0, 1)
        ]
        for copy in copies:
            copy.start()
        for copy in copies:
            copy.wait()


def solution(mesh):
    n = mesh.shape[AXIS]

    def step(x, w_gate, w_up, w_down):
        tokens, d_model = x.shape
        hidden = w_gate.shape[1]
        block = tokens // n
        up_tile, down_tile = 256, 256
        up_tiles, down_tiles = hidden // up_tile, d_model // down_tile
        y = pl.pallas_call(
            functools.partial(kernel, n),
            out_shape=pltpu.VMEM((tokens, d_model), jnp.bfloat16),
            in_specs=[pl.BlockSpec(memory_space=pl.ANY)] * 4,
            out_specs=pl.BlockSpec(memory_space=pltpu.VMEM),
            scratch_shapes=[
                pltpu.VMEM((block, d_model), jnp.bfloat16),
                pltpu.VMEM((up_tiles, d_model, up_tile), jnp.bfloat16),
                pltpu.VMEM((up_tiles, d_model, up_tile), jnp.bfloat16),
                pltpu.VMEM((down_tiles, hidden, down_tile), jnp.bfloat16),
                pltpu.VMEM((block, hidden), jnp.bfloat16),
                pltpu.SemaphoreType.DMA((2, 2)),
                pltpu.SemaphoreType.DMA((2, up_tiles)),
                pltpu.SemaphoreType.DMA((down_tiles,)),
                pltpu.SemaphoreType.DMA((2, down_tiles)),
                pltpu.SemaphoreType.DMA((2, 2, down_tiles)),
                pltpu.SemaphoreType.DMA((up_tiles + 1,)),
                pltpu.SemaphoreType.DMA((up_tiles + 1,)),
                pltpu.SemaphoreType.REGULAR,
            ],
            compiler_params=pltpu.CompilerParams(
                collective_id=0, has_side_effects=True, vmem_limit_bytes=50_200_000
            ),
            name="mlp_ring",
        )(x, w_gate, w_up, w_down)
        in_vmem, anywhere = pl.BlockSpec(memory_space=pltpu.VMEM), pl.BlockSpec(memory_space=pl.ANY)
        y = pltpu.with_memory_space_constraint(y, pltpu.VMEM)
        whole = jax.ShapeDtypeStruct((tokens, d_model), jnp.bfloat16)
        out = pl.pallas_call(
            functools.partial(write_gathered, n),
            out_shape=whole,
            in_specs=[in_vmem],
            out_specs=anywhere,
            scratch_shapes=[pltpu.SemaphoreType.DMA((2, n))],
            compiler_params=pltpu.CompilerParams(vmem_limit_bytes=1 << 20),
            name="write_gathered",
        )(y)
        held = pl.pallas_call(
            functools.partial(last_hop, n),
            out_shape=pltpu.VMEM((2, block // 2, d_model), jnp.bfloat16),
            in_specs=[in_vmem, pl.BlockSpec(memory_space=pltpu.HBM)],
            out_specs=in_vmem,
            scratch_shapes=[pltpu.SemaphoreType.DMA((2,)), pltpu.SemaphoreType.DMA((2,))],
            compiler_params=pltpu.CompilerParams(collective_id=1, has_side_effects=True, vmem_limit_bytes=1 << 20),
            name="last_hop",
        )(y, pltpu.with_memory_space_constraint(out, pltpu.HBM))
        return pl.pallas_call(
            functools.partial(write_last, n),
            out_shape=whole,
            in_specs=[in_vmem, anywhere],
            out_specs=anywhere,
            scratch_shapes=[pltpu.SemaphoreType.DMA((2,))],
            input_output_aliases={1: 0},
            compiler_params=pltpu.CompilerParams(vmem_limit_bytes=1 << 20),
            name="write_last",
        )(pltpu.with_memory_space_constraint(held, pltpu.VMEM), out)

    return jax.shard_map(
        step,
        mesh=mesh,
        in_specs=(P("dp", None), P(None, AXIS), P(None, AXIS), P(AXIS, None)),
        out_specs=P("dp", None),
        check_vma=False,
    )
```

```python
import functools

import jax
import jax.numpy as jnp
from jax import lax
from jax.experimental import pallas as pl
from jax.experimental.pallas import tpu as pltpu
from jax.sharding import PartitionSpec as P

MESH = pl.DeviceIdType.MESH
AXIS, GROUPS = "tp", "dp"


def gathered(n):
    return n - 2 + lax.rem(lax.axis_index(GROUPS), 2)


def half_rows(half, direction, j):
    return pl.ds(pl.multiple_of(j * 2 * half + direction * half, half), half)


def greet(*others):
    barrier = pltpu.get_barrier_semaphore()
    for other in others:
        pl.semaphore_signal(barrier, inc=1, device_id=other, device_id_type=MESH)
    return barrier


def kernel(
    n,
    x_hbm,
    wg_hbm,
    wu_hbm,
    wd_hbm,
    y,
    xv,
    wg,
    wu,
    wd,
    hidden,
    x_sem,
    up_sem,
    send_sem,
    recv_sem,
    share_send,
    share_recv,
    told,
):
    me = lax.axis_index(AXIS)
    right, left = lax.rem(me + 1, n), lax.rem(me + n - 1, n)
    half = xv.shape[0] // 2
    part = half // 2
    up_tiles, _, up_tile = wg.shape
    down_tiles, _, down_tile = wd.shape
    group = lax.axis_index(GROUPS)
    core = lax.rem(group, 2)
    partner = {GROUPS: group + 1 - 2 * core}
    shared = up_tiles // 2
    first, theirs = core * (up_tiles - shared), (1 - core) * (up_tiles - shared)
    between = range(shared, up_tiles - shared)
    own, other = pl.ds(0, 2 * part), pl.ds(2 * part, 2 * part)

    def shard(direction, step):
        if direction == 0:
            return lax.rem(me + 2 * n - 1 - step, n)
        return lax.rem(me + 1 + step, n)

    def part_rows(direction, j, p):
        return pl.ds(pl.multiple_of(j * 2 * half + direction * half + p * part, part), part)

    def tile_columns(t, size):
        return pl.ds(pl.multiple_of(t * size, size), size)

    def x_copies(step, p):
        return [
            pltpu.make_async_copy(
                x_hbm.at[part_rows(d, shard(d, step), p), :],
                xv.at[pl.ds((2 * p + d) * part, part), :],
                x_sem.at[d, p],
            )
            for d in (0, 1)
        ]

    def up_copies(t, slot):
        return [
            pltpu.make_async_copy(hbm.at[:, tile_columns(t, up_tile)], vmem.at[t], up_sem.at[k, slot])
            for k, (hbm, vmem) in enumerate(((wg_hbm, wg), (wu_hbm, wu)))
        ]

    def down_copy(t):
        return pltpu.make_async_copy(wd_hbm.at[:, tile_columns(t, down_tile)], wd.at[t], send_sem.at[0, t])

    def send(direction, block, t, count):
        return pltpu.make_async_remote_copy(
            src_ref=block,
            dst_ref=block,
            send_sem=send_sem.at[direction, t],
            recv_sem=recv_sem.at[direction, lax.rem(count, 2), t],
            device_id={AXIS: right if direction == 0 else left},
            device_id_type=MESH,
        )

    def hop(direction, j, t, count):
        return send(direction, y.at[half_rows(half, direction, j), tile_columns(t, down_tile)], t, count)

    def first_hop(direction, p, t):
        rows = part_rows(direction, shard(direction, 0), p)
        return send(direction, y.at[rows, tile_columns(t, down_tile)], t, 0)

    def each_tile(low, high, act):
        def tile(t, _):
            act(t)
            return 0

        lax.fori_loop(low, high, tile, 0)

    def start_up(t, slot):
        for copy in up_copies(t, slot):
            copy.start()

    def wait_up(t, slot):
        for copy in up_copies(t, slot):
            copy.wait()

    def share(src, dst, k):
        return pltpu.make_async_remote_copy(
            src_ref=src,
            dst_ref=dst,
            send_sem=share_send.at[k],
            recv_sem=share_recv.at[k],
            device_id=partner,
            device_id_type=MESH,
        )

    def share_x():
        return share(xv.at[own, :], xv.at[other, :], shared)

    def share_hidden(base, k):
        columns = tile_columns(base + k, up_tile)
        return share(hidden.at[other, columns], hidden.at[own, columns], k)

    def up_tile_of(rows, t):
        gate = jnp.dot(xv[rows, :], wg[t], preferred_element_type=jnp.float32)
        up = jnp.dot(xv[rows, :], wu[t], preferred_element_type=jnp.float32)
        hidden[rows, tile_columns(t, up_tile)] = (jax.nn.silu(gate) * up).astype(hidden.dtype)

    def project_up():
        each_tile(0, up_tiles, lambda t: up_tile_of(pl.ds(0, 2 * half), t))

    def project_second_up():
        for t in [first + k for k in range(shared)] + list(between):
            up_tile_of(other, t)
        each_tile(0, shared, lambda k: wait_up(theirs + k, k))
        each_tile(theirs, theirs + shared, lambda t: up_tile_of(other, t))

    def project_shared():
        last = first + shared - 1
        wait_up(first, 0)
        up_tile_of(own, first)
        share_x().wait_recv()
        up_tile_of(other, first)

        def tile(t, _):
            wait_up(t, t - first)
            up_tile_of(pl.ds(0, 2 * half), t)
            share_hidden(first, t - 1 - first).start()
            return 0

        lax.fori_loop(first + 1, last, tile, 0)
        wait_up(last, shared - 1)
        up_tile_of(other, last)
        for k in (shared - 2, shared - 1):
            share_hidden(first, k).start()

        @pl.when(core == 1)
        def _():
            pl.semaphore_wait(barrier, 4)
            pl.semaphore_signal(told, inc=1, device_id=partner, device_id_type=MESH)

        up_tile_of(own, last)
        for t in between:
            wait_up(t, t)
            up_tile_of(own, t)

    def project_first_down(p):
        rows = pl.ds(2 * p * part, 2 * part)
        singles = 4 if p == 0 else 2

        def start(t):
            for d in (0, 1):
                first_hop(d, p, t).start()

        def tiles(ts):
            if p == 0:
                for t in ts:
                    down_copy(t).wait()
            for t in ts:
                term = jnp.dot(hidden[rows, :], wd[t], preferred_element_type=jnp.float32)
                for d in (0, 1):
                    y[part_rows(d, shard(d, 0), p), tile_columns(t, down_tile)] = term[
                        d * part : (d + 1) * part, :
                    ].astype(y.dtype)

        def single(t, _):
            tiles((t,))
            start(t - 1)
            return 0

        def pair(g, _):
            tiles((2 * g, 2 * g + 1))

            @pl.when(2 * g > singles)
            def _():
                start(2 * g - 2)

            start(2 * g - 1)
            return 0

        tiles((0,))
        lax.fori_loop(1, singles, single, 0)
        lax.fori_loop(singles // 2, down_tiles // 2, pair, 0)
        start(down_tiles - 2)
        start(down_tiles - 1)

    def project_down(step):
        js = [shard(d, step) for d in (0, 1)]
        before = [shard(d, step - 1) for d in (0, 1)]

        def tile(t, _):
            columns = tile_columns(t, down_tile)
            term = jnp.dot(hidden[...], wd[t], preferred_element_type=jnp.float32)
            for d in (0, 1):
                hop(d, js[d], t, step - 1).wait_recv()
                hop(d, before[d], t, step - 1).wait_send()
            for d in (0, 1):
                for p in (0, 1):
                    rows = part_rows(d, js[d], p)
                    own = term[(2 * p + d) * part : (2 * p + d + 1) * part, :]
                    y[rows, columns] = (own + y[rows, columns].astype(jnp.float32)).astype(y.dtype)

            @pl.when(t > 0)
            def _():
                for d in (0, 1):
                    hop(d, js[d], t - 1, step).start()

            return 0

        lax.fori_loop(0, down_tiles, tile, 0)
        for d in (0, 1):
            hop(d, js[d], down_tiles - 1, step).start()

    listener = group - core + 1
    barrier = greet({AXIS: left, GROUPS: listener}, {AXIS: right, GROUPS: listener})

    @pl.when(core == 1)
    def _():
        pl.semaphore_signal(barrier, inc=1, device_id=partner, device_id_type=MESH)

    for copy in x_copies(0, 0):
        copy.start()
    each_tile(0, shared, lambda k: start_up(first + k, k))
    for t in between:
        start_up(t, t)
    each_tile(0, down_tiles, lambda t: down_copy(t).start())

    @pl.when(core == 0)
    def _():
        pl.semaphore_wait(barrier, 1)
        pl.semaphore_signal(told, inc=1, device_id=partner, device_id_type=MESH)

    @pl.when(core == 1)
    def _():
        pl.semaphore_wait(told, 1)

    for copy in x_copies(0, 0):
        copy.wait()
    share_x().start()
    project_shared()

    @pl.when(core == 0)
    def _():
        pl.semaphore_wait(told, 1)

    for copy in x_copies(0, 1):
        copy.start()
    each_tile(0, shared, lambda k: start_up(theirs + k, k))
    each_tile(0, shared, lambda k: share_hidden(theirs, k).wait_recv())
    project_first_down(0)

    for copy in x_copies(0, 1):
        copy.wait()
    share_x().wait_send()
    each_tile(0, shared, lambda k: share_hidden(first, k).wait_send())
    for copy in x_copies(1, 0):
        copy.start()
    project_second_up()
    for copy in x_copies(1, 1):
        copy.start()
    project_first_down(1)

    def reduce_step(step, _):
        for p in (0, 1):
            for copy in x_copies(step, p):
                copy.wait()
        project_up()

        @pl.when(step < n - 1)
        def _():
            for p in (0, 1):
                for copy in x_copies(step + 1, p):
                    copy.start()

        project_down(step)
        return 0

    lax.fori_loop(1, n, reduce_step, 0)

    last = gathered(n)

    def gather_step(step, _):
        js = [lax.rem(me + n - step, n), lax.rem(me + step, n)]
        before = [lax.rem(me + n - step + 1, n), lax.rem(me + step - 1, n)]

        def tile(t, _):
            for d in (0, 1):
                hop(d, js[d], t, n - 2 + step).wait_recv()
                hop(d, before[d], t, n - 2 + step).wait_send()

            @pl.when(step < last)
            def _():
                for d in (0, 1):
                    hop(d, js[d], t, n - 1 + step).start()

            return 0

        return lax.fori_loop(0, down_tiles, tile, 0)

    lax.fori_loop(1, last + 1, gather_step, 0)


def write_gathered(n, y, out, sem):
    me = lax.axis_index(AXIS)
    last = gathered(n)
    half = y.shape[0] // (2 * n)

    def each(act):
        def step(a, _):
            for d, j in enumerate((lax.rem(me + n - a, n), lax.rem(me + a, n))):
                block = half_rows(half, d, j)
                act(pltpu.make_async_copy(y.at[block, :], out.at[block, :], sem.at[d, a]))
            return 0

        lax.fori_loop(0, last + 1, step, 0)

    each(lambda copy: copy.start())
    each(lambda copy: copy.wait())


def last_hop(n, y, _, held, send_sem, recv_sem):
    me = lax.axis_index(AXIS)
    half = held.shape[1]
    neighbours = (lax.rem(me + 1, n), lax.rem(me + n - 1, n))
    js = (lax.rem(me + 2, n), lax.rem(me + n - 2, n))

    @pl.when(gathered(n) < n - 1)
    def _():
        barrier = greet({AXIS: neighbours[0]}, {AXIS: neighbours[1]})
        pl.semaphore_wait(barrier, 2)
        hops = [
            pltpu.make_async_remote_copy(
                src_ref=y.at[half_rows(half, d, js[d]), :],
                dst_ref=held.at[d],
                send_sem=send_sem.at[d],
                recv_sem=recv_sem.at[d],
                device_id={AXIS: neighbours[d]},
                device_id_type=MESH,
            )
            for d in (0, 1)
        ]
        for hop in hops:
            hop.start()
        for hop in hops:
            hop.wait()


def write_last(n, held, _, out, sem):
    me = lax.axis_index(AXIS)
    half = held.shape[1]
    js = (lax.rem(me + 1, n), lax.rem(me + n - 1, n))

    @pl.when(gathered(n) < n - 1)
    def _():
        copies = [
            pltpu.make_async_copy(held.at[d], out.at[half_rows(half, d, js[d]), :], sem.at[d]) for d in (0, 1)
        ]
        for copy in copies:
            copy.start()
        for copy in copies:
            copy.wait()


def solution(mesh):
    n = mesh.shape[AXIS]

    def step(x, w_gate, w_up, w_down):
        tokens, d_model = x.shape
        hidden = w_gate.shape[1]
        block = tokens // n
        up_tile, down_tile = 256, 256
        up_tiles, down_tiles = hidden // up_tile, d_model // down_tile
        y = pl.pallas_call(
            functools.partial(kernel, n),
            out_shape=pltpu.VMEM((tokens, d_model), jnp.bfloat16),
            in_specs=[pl.BlockSpec(memory_space=pl.ANY)] * 4,
            out_specs=pl.BlockSpec(memory_space=pltpu.VMEM),
            scratch_shapes=[
                pltpu.VMEM((block, d_model), jnp.bfloat16),
                pltpu.VMEM((up_tiles, d_model, up_tile), jnp.bfloat16),
                pltpu.VMEM((up_tiles, d_model, up_tile), jnp.bfloat16),
                pltpu.VMEM((down_tiles, hidden, down_tile), jnp.bfloat16),
                pltpu.VMEM((block, hidden), jnp.bfloat16),
                pltpu.SemaphoreType.DMA((2, 2)),
                pltpu.SemaphoreType.DMA((2, up_tiles - up_tiles // 2)),
                pltpu.SemaphoreType.DMA((2, down_tiles)),
                pltpu.SemaphoreType.DMA((2, 2, down_tiles)),
                pltpu.SemaphoreType.DMA((up_tiles // 2 + 1,)),
                pltpu.SemaphoreType.DMA((up_tiles // 2 + 1,)),
                pltpu.SemaphoreType.REGULAR,
            ],
            compiler_params=pltpu.CompilerParams(
                collective_id=0, has_side_effects=True, vmem_limit_bytes=50_200_000
            ),
            name="mlp_ring",
        )(x, w_gate, w_up, w_down)
        in_vmem, anywhere = pl.BlockSpec(memory_space=pltpu.VMEM), pl.BlockSpec(memory_space=pl.ANY)
        y = pltpu.with_memory_space_constraint(y, pltpu.VMEM)
        whole = jax.ShapeDtypeStruct((tokens, d_model), jnp.bfloat16)
        out = pl.pallas_call(
            functools.partial(write_gathered, n),
            out_shape=whole,
            in_specs=[in_vmem],
            out_specs=anywhere,
            scratch_shapes=[pltpu.SemaphoreType.DMA((2, n))],
            compiler_params=pltpu.CompilerParams(vmem_limit_bytes=1 << 20),
            name="write_gathered",
        )(y)
        held = pl.pallas_call(
            functools.partial(last_hop, n),
            out_shape=pltpu.VMEM((2, block // 2, d_model), jnp.bfloat16),
            in_specs=[in_vmem, pl.BlockSpec(memory_space=pltpu.HBM)],
            out_specs=in_vmem,
            scratch_shapes=[pltpu.SemaphoreType.DMA((2,)), pltpu.SemaphoreType.DMA((2,))],
            compiler_params=pltpu.CompilerParams(collective_id=1, has_side_effects=True, vmem_limit_bytes=1 << 20),
            name="last_hop",
        )(y, pltpu.with_memory_space_constraint(out, pltpu.HBM))
        return pl.pallas_call(
            functools.partial(write_last, n),
            out_shape=whole,
            in_specs=[in_vmem, anywhere],
            out_specs=anywhere,
            scratch_shapes=[pltpu.SemaphoreType.DMA((2,))],
            input_output_aliases={1: 0},
            compiler_params=pltpu.CompilerParams(vmem_limit_bytes=1 << 20),
            name="write_last",
        )(pltpu.with_memory_space_constraint(held, pltpu.VMEM), out)

    return jax.shard_map(
        step,
        mesh=mesh,
        in_specs=(P("dp", None), P(None, AXIS), P(None, AXIS), P(AXIS, None)),
        out_specs=P("dp", None),
        check_vma=False,
    )
```

```python
import functools

import jax
import jax.numpy as jnp
from jax import lax
from jax.experimental import pallas as pl
from jax.experimental.pallas import tpu as pltpu
from jax.sharding import PartitionSpec as P

MESH = pl.DeviceIdType.MESH
AXIS, GROUPS = "tp", "dp"


def gathered(n):
    return n - 2 + lax.rem(lax.axis_index(GROUPS), 2)


def half_rows(half, direction, j):
    return pl.ds(pl.multiple_of(j * 2 * half + direction * half, half), half)


def greet(*others):
    barrier = pltpu.get_barrier_semaphore()
    for other in others:
        pl.semaphore_signal(barrier, inc=1, device_id=other, device_id_type=MESH)
    return barrier


def kernel(
    n,
    x_hbm,
    wg_hbm,
    wu_hbm,
    wd_hbm,
    y,
    xv,
    wg,
    wu,
    wd,
    hidden,
    x_sem,
    up_sem,
    send_sem,
    recv_sem,
    share_send,
    share_recv,
    told,
):
    me = lax.axis_index(AXIS)
    right, left = lax.rem(me + 1, n), lax.rem(me + n - 1, n)
    half = xv.shape[0] // 2
    part = half // 2
    up_tiles, _, up_tile = wg.shape
    down_tiles, _, down_tile = wd.shape
    group = lax.axis_index(GROUPS)
    core = lax.rem(group, 2)
    partner = {GROUPS: group + 1 - 2 * core}
    shared = up_tiles // 2
    first, theirs = core * (up_tiles - shared), (1 - core) * (up_tiles - shared)
    between = range(shared, up_tiles - shared)
    own, other = pl.ds(0, 2 * part), pl.ds(2 * part, 2 * part)

    def shard(direction, step):
        if direction == 0:
            return lax.rem(me + 2 * n - 1 - step, n)
        return lax.rem(me + 1 + step, n)

    def part_rows(direction, j, p):
        return pl.ds(pl.multiple_of(j * 2 * half + direction * half + p * part, part), part)

    def tile_columns(t, size):
        return pl.ds(pl.multiple_of(t * size, size), size)

    def x_copies(step, p):
        return [
            pltpu.make_async_copy(
                x_hbm.at[part_rows(d, shard(d, step), p), :],
                xv.at[pl.ds((2 * p + d) * part, part), :],
                x_sem.at[d, p],
            )
            for d in (0, 1)
        ]

    def up_copies(t, slot):
        return [
            pltpu.make_async_copy(hbm.at[:, tile_columns(t, up_tile)], vmem.at[t], up_sem.at[k, slot])
            for k, (hbm, vmem) in enumerate(((wg_hbm, wg), (wu_hbm, wu)))
        ]

    def down_copy(t):
        return pltpu.make_async_copy(wd_hbm.at[:, tile_columns(t, down_tile)], wd.at[t], send_sem.at[0, t])

    def send(direction, block, t, count):
        return pltpu.make_async_remote_copy(
            src_ref=block,
            dst_ref=block,
            send_sem=send_sem.at[direction, t],
            recv_sem=recv_sem.at[direction, lax.rem(count, 2), t],
            device_id={AXIS: right if direction == 0 else left},
            device_id_type=MESH,
        )

    def hop(direction, j, t, count):
        return send(direction, y.at[half_rows(half, direction, j), tile_columns(t, down_tile)], t, count)

    def first_hop(direction, p, t):
        rows = part_rows(direction, shard(direction, 0), p)
        return send(direction, y.at[rows, tile_columns(t, down_tile)], t, 0)

    def each_tile(low, high, act):
        def tile(t, _):
            act(t)
            return 0

        lax.fori_loop(low, high, tile, 0)

    def start_up(t, slot):
        for copy in up_copies(t, slot):
            copy.start()

    def wait_up(t, slot):
        for copy in up_copies(t, slot):
            copy.wait()

    def share(src, dst, k):
        return pltpu.make_async_remote_copy(
            src_ref=src,
            dst_ref=dst,
            send_sem=share_send.at[k],
            recv_sem=share_recv.at[k],
            device_id=partner,
            device_id_type=MESH,
        )

    def share_x():
        return share(xv.at[own, :], xv.at[other, :], shared)

    def share_hidden(base, k):
        columns = tile_columns(base + k, up_tile)
        return share(hidden.at[other, columns], hidden.at[own, columns], k)

    def up_tile_of(rows, t):
        gate = jnp.dot(xv[rows, :], wg[t], preferred_element_type=jnp.float32)
        up = jnp.dot(xv[rows, :], wu[t], preferred_element_type=jnp.float32)
        hidden[rows, tile_columns(t, up_tile)] = (jax.nn.silu(gate) * up).astype(hidden.dtype)

    def project_up():
        each_tile(0, up_tiles, lambda t: up_tile_of(pl.ds(0, 2 * half), t))

    def project_second_up():
        for t in [first + k for k in range(shared)] + list(between):
            up_tile_of(other, t)
        each_tile(0, shared, lambda k: wait_up(theirs + k, k))
        each_tile(theirs, theirs + shared, lambda t: up_tile_of(other, t))

    def project_shared():
        last = first + shared - 1
        wait_up(first, 0)
        up_tile_of(own, first)
        share_x().wait_recv()
        up_tile_of(other, first)

        def tile(t, _):
            wait_up(t, t - first)
            up_tile_of(pl.ds(0, 2 * half), t)
            share_hidden(first, t - 1 - first).start()
            return 0

        lax.fori_loop(first + 1, last, tile, 0)
        wait_up(last, shared - 1)
        up_tile_of(other, last)
        for k in (shared - 2, shared - 1):
            share_hidden(first, k).start()

        @pl.when(core == 1)
        def _():
            pl.semaphore_wait(barrier, 4)
            pl.semaphore_signal(told, inc=1, device_id=partner, device_id_type=MESH)

        up_tile_of(own, last)
        for t in between:
            wait_up(t, t)
            up_tile_of(own, t)

    def project_first_down(p):
        rows = pl.ds(2 * p * part, 2 * part)
        singles = 4 if p == 0 else 2

        def start(t):
            for d in (0, 1):
                first_hop(d, p, t).start()

        def tiles(ts):
            if p == 0:
                for t in ts:
                    down_copy(t).wait()
            for t in ts:
                term = jnp.dot(hidden[rows, :], wd[t], preferred_element_type=jnp.float32)
                for d in (0, 1):
                    y[part_rows(d, shard(d, 0), p), tile_columns(t, down_tile)] = term[
                        d * part : (d + 1) * part, :
                    ].astype(y.dtype)

        def single(t, _):
            tiles((t,))
            start(t - 1)
            return 0

        def pair(g, _):
            tiles((2 * g, 2 * g + 1))

            @pl.when(2 * g > singles)
            def _():
                start(2 * g - 2)

            start(2 * g - 1)
            return 0

        tiles((0,))
        lax.fori_loop(1, singles, single, 0)
        lax.fori_loop(singles // 2, down_tiles // 2, pair, 0)
        start(down_tiles - 2)
        start(down_tiles - 1)

    def project_down(step):
        js = [shard(d, step) for d in (0, 1)]
        before = [shard(d, step - 1) for d in (0, 1)]

        def tile(t, _):
            columns = tile_columns(t, down_tile)
            term = jnp.dot(hidden[...], wd[t], preferred_element_type=jnp.float32)
            for d in (0, 1):
                hop(d, js[d], t, step - 1).wait_recv()
                hop(d, before[d], t, step - 1).wait_send()
            for d in (0, 1):
                for p in (0, 1):
                    rows = part_rows(d, js[d], p)
                    own = term[(2 * p + d) * part : (2 * p + d + 1) * part, :]
                    y[rows, columns] = (own + y[rows, columns].astype(jnp.float32)).astype(y.dtype)

            @pl.when(t > 0)
            def _():
                for d in (0, 1):
                    hop(d, js[d], t - 1, step).start()

            return 0

        lax.fori_loop(0, down_tiles, tile, 0)
        for d in (0, 1):
            hop(d, js[d], down_tiles - 1, step).start()

    for copy in x_copies(0, 0):
        copy.start()
    each_tile(0, shared, lambda k: start_up(first + k, k))
    for t in between:
        start_up(t, t)

    listener = group - core + 1
    barrier = greet({AXIS: left, GROUPS: listener}, {AXIS: right, GROUPS: listener})

    @pl.when(core == 1)
    def _():
        pl.semaphore_signal(barrier, inc=1, device_id=partner, device_id_type=MESH)

    each_tile(0, down_tiles, lambda t: down_copy(t).start())

    @pl.when(core == 0)
    def _():
        pl.semaphore_wait(barrier, 1)
        pl.semaphore_signal(told, inc=1, device_id=partner, device_id_type=MESH)

    @pl.when(core == 1)
    def _():
        pl.semaphore_wait(told, 1)

    for copy in x_copies(0, 0):
        copy.wait()
    share_x().start()
    project_shared()

    @pl.when(core == 0)
    def _():
        pl.semaphore_wait(told, 1)

    for copy in x_copies(0, 1):
        copy.start()
    each_tile(0, shared, lambda k: start_up(theirs + k, k))
    each_tile(0, shared, lambda k: share_hidden(theirs, k).wait_recv())
    project_first_down(0)

    for copy in x_copies(0, 1):
        copy.wait()
    share_x().wait_send()
    each_tile(0, shared, lambda k: share_hidden(first, k).wait_send())
    for copy in x_copies(1, 0):
        copy.start()
    project_second_up()
    for copy in x_copies(1, 1):
        copy.start()
    project_first_down(1)

    def reduce_step(step, _):
        for p in (0, 1):
            for copy in x_copies(step, p):
                copy.wait()
        project_up()

        @pl.when(step < n - 1)
        def _():
            for p in (0, 1):
                for copy in x_copies(step + 1, p):
                    copy.start()

        project_down(step)
        return 0

    lax.fori_loop(1, n, reduce_step, 0)

    last = gathered(n)

    def gather_step(step, _):
        js = [lax.rem(me + n - step, n), lax.rem(me + step, n)]
        before = [lax.rem(me + n - step + 1, n), lax.rem(me + step - 1, n)]

        def tile(t, _):
            for d in (0, 1):
                hop(d, js[d], t, n - 2 + step).wait_recv()
                hop(d, before[d], t, n - 2 + step).wait_send()

            @pl.when(step < last)
            def _():
                for d in (0, 1):
                    hop(d, js[d], t, n - 1 + step).start()

            return 0

        return lax.fori_loop(0, down_tiles, tile, 0)

    lax.fori_loop(1, last + 1, gather_step, 0)


def write_gathered(n, y, out, sem):
    me = lax.axis_index(AXIS)
    last = gathered(n)
    half = y.shape[0] // (2 * n)

    def each(act):
        def step(a, _):
            for d, j in enumerate((lax.rem(me + n - a, n), lax.rem(me + a, n))):
                block = half_rows(half, d, j)
                act(pltpu.make_async_copy(y.at[block, :], out.at[block, :], sem.at[d, a]))
            return 0

        lax.fori_loop(0, last + 1, step, 0)

    each(lambda copy: copy.start())
    each(lambda copy: copy.wait())


def last_hop(n, y, _, held, send_sem, recv_sem):
    me = lax.axis_index(AXIS)
    half = held.shape[1]
    neighbours = (lax.rem(me + 1, n), lax.rem(me + n - 1, n))
    js = (lax.rem(me + 2, n), lax.rem(me + n - 2, n))

    @pl.when(gathered(n) < n - 1)
    def _():
        barrier = greet({AXIS: neighbours[0]}, {AXIS: neighbours[1]})
        pl.semaphore_wait(barrier, 2)
        hops = [
            pltpu.make_async_remote_copy(
                src_ref=y.at[half_rows(half, d, js[d]), :],
                dst_ref=held.at[d],
                send_sem=send_sem.at[d],
                recv_sem=recv_sem.at[d],
                device_id={AXIS: neighbours[d]},
                device_id_type=MESH,
            )
            for d in (0, 1)
        ]
        for hop in hops:
            hop.start()
        for hop in hops:
            hop.wait()


def write_last(n, held, _, out, sem):
    me = lax.axis_index(AXIS)
    half = held.shape[1]
    js = (lax.rem(me + 1, n), lax.rem(me + n - 1, n))

    @pl.when(gathered(n) < n - 1)
    def _():
        copies = [
            pltpu.make_async_copy(held.at[d], out.at[half_rows(half, d, js[d]), :], sem.at[d]) for d in (0, 1)
        ]
        for copy in copies:
            copy.start()
        for copy in copies:
            copy.wait()


def solution(mesh):
    n = mesh.shape[AXIS]

    def step(x, w_gate, w_up, w_down):
        tokens, d_model = x.shape
        hidden = w_gate.shape[1]
        block = tokens // n
        up_tile, down_tile = 256, 256
        up_tiles, down_tiles = hidden // up_tile, d_model // down_tile
        y = pl.pallas_call(
            functools.partial(kernel, n),
            out_shape=pltpu.VMEM((tokens, d_model), jnp.bfloat16),
            in_specs=[pl.BlockSpec(memory_space=pl.ANY)] * 4,
            out_specs=pl.BlockSpec(memory_space=pltpu.VMEM),
            scratch_shapes=[
                pltpu.VMEM((block, d_model), jnp.bfloat16),
                pltpu.VMEM((up_tiles, d_model, up_tile), jnp.bfloat16),
                pltpu.VMEM((up_tiles, d_model, up_tile), jnp.bfloat16),
                pltpu.VMEM((down_tiles, hidden, down_tile), jnp.bfloat16),
                pltpu.VMEM((block, hidden), jnp.bfloat16),
                pltpu.SemaphoreType.DMA((2, 2)),
                pltpu.SemaphoreType.DMA((2, up_tiles - up_tiles // 2)),
                pltpu.SemaphoreType.DMA((2, down_tiles)),
                pltpu.SemaphoreType.DMA((2, 2, down_tiles)),
                pltpu.SemaphoreType.DMA((up_tiles // 2 + 1,)),
                pltpu.SemaphoreType.DMA((up_tiles // 2 + 1,)),
                pltpu.SemaphoreType.REGULAR,
            ],
            compiler_params=pltpu.CompilerParams(
                collective_id=0, has_side_effects=True, vmem_limit_bytes=50_200_000
            ),
            name="mlp_ring",
        )(x, w_gate, w_up, w_down)
        in_vmem, anywhere = pl.BlockSpec(memory_space=pltpu.VMEM), pl.BlockSpec(memory_space=pl.ANY)
        y = pltpu.with_memory_space_constraint(y, pltpu.VMEM)
        whole = jax.ShapeDtypeStruct((tokens, d_model), jnp.bfloat16)
        out = pl.pallas_call(
            functools.partial(write_gathered, n),
            out_shape=whole,
            in_specs=[in_vmem],
            out_specs=anywhere,
            scratch_shapes=[pltpu.SemaphoreType.DMA((2, n))],
            compiler_params=pltpu.CompilerParams(vmem_limit_bytes=1 << 20),
            name="write_gathered",
        )(y)
        held = pl.pallas_call(
            functools.partial(last_hop, n),
            out_shape=pltpu.VMEM((2, block // 2, d_model), jnp.bfloat16),
            in_specs=[in_vmem, pl.BlockSpec(memory_space=pltpu.HBM)],
            out_specs=in_vmem,
            scratch_shapes=[pltpu.SemaphoreType.DMA((2,)), pltpu.SemaphoreType.DMA((2,))],
            compiler_params=pltpu.CompilerParams(collective_id=1, has_side_effects=True, vmem_limit_bytes=1 << 20),
            name="last_hop",
        )(y, pltpu.with_memory_space_constraint(out, pltpu.HBM))
        return pl.pallas_call(
            functools.partial(write_last, n),
            out_shape=whole,
            in_specs=[in_vmem, anywhere],
            out_specs=anywhere,
            scratch_shapes=[pltpu.SemaphoreType.DMA((2,))],
            input_output_aliases={1: 0},
            compiler_params=pltpu.CompilerParams(vmem_limit_bytes=1 << 20),
            name="write_last",
        )(pltpu.with_memory_space_constraint(held, pltpu.VMEM), out)

    return jax.shard_map(
        step,
        mesh=mesh,
        in_specs=(P("dp", None), P(None, AXIS), P(None, AXIS), P(AXIS, None)),
        out_specs=P("dp", None),
        check_vma=False,
    )
```
